16 devices in a mesh: dp: 2 (over y, z), tp: 8 (over x, core).
Axes of the slice: x: 4, y: 2, z: 1, core: 2. Of those that a mesh axis runs over, the one named last changes fastest.
The devices are a block of a 4x4x4 slice.
Arguments:
- x: bfloat16 [8, 512, 8192], P('dp'), parts along dimension 0
- gain_a: bfloat16 [8192], replicated
- wq: bfloat16 [8192, 8192], P(None, 'tp')
- wk: bfloat16 [8192, 1024], P(None, 'tp')
- wv: bfloat16 [8192, 1024], P(None, 'tp')
- wo: bfloat16 [8192, 8192], P('tp')
- gain_m: bfloat16 [8192], replicated
- w_gate: bfloat16 [8192, 49152], P(None, 'tp')
- w_up: bfloat16 [8192, 49152], P(None, 'tp')
- w_down: bfloat16 [49152, 8192], P('tp')
Outputs:
- output: bfloat16 [8, 512, 8192], P('dp'), parts along dimension 0
There are 2 independent parts. The reference program is written for one: setup_inputs(seed, part) draws one part's arguments, and reference() takes and returns one part's arrays. A program takes and returns all parts, laid end to end along the dimension named above; an argument that names none is the same for every part.
All inputs are finite; a program needn't handle non-finite values.
Results may differ from the reference program's by a relative error of at most 0.017.
Values are sent between devices in bfloat16 or wider.
A program may use at most 1.5 GiB of HBM per device.

```python
import jax
import jax.numpy as jnp
from jax import lax

SEQUENCES = 4
TOKENS = 512
D = 8192
HEADS = 64
KV_HEADS = 8
HEAD = 128
FF = 49152
THETA = 10000


def setup_inputs(seed: int = 0, part: int = 0) -> dict:
    kx, ka, km, kq, kk, kv, ko, kg, ku, kd = jax.random.split(jax.random.key(seed), 10)

    def weights(key, rows, columns):
        return jax.random.normal(key, (rows, columns), jnp.float32) * rows**-0.5

    drawn = {
        "x": jax.random.normal(jax.random.fold_in(kx, part), (SEQUENCES, TOKENS, D), jnp.float32),
        "gain_a": 1 + 0.1 * jax.random.normal(ka, (D,), jnp.float32),
        "wq": 2 * weights(kq, D, HEADS * HEAD),
        "wk": 2 * weights(kk, D, KV_HEADS * HEAD),
        "wv": 4 * weights(kv, D, KV_HEADS * HEAD),
        "wo": weights(ko, HEADS * HEAD, D),
        "gain_m": 1 + 0.1 * jax.random.normal(km, (D,), jnp.float32),
        "w_gate": weights(kg, D, FF),
        "w_up": weights(ku, D, FF),
        "w_down": 3 * weights(kd, FF, D),
    }
    return {k: v.astype(jnp.bfloat16) for k, v in drawn.items()}


def normed(x, gain):
    wide = x.astype(jnp.float32)
    scale = lax.rsqrt(jnp.mean(wide * wide, -1, keepdims=True) + 1e-6)
    return (wide * scale * gain.astype(jnp.float32)).astype(jnp.bfloat16)


def turned(t, place, theta):
    half = t.shape[-1] // 2
    angle = place.astype(jnp.float32)[:, None] * theta ** (-jnp.arange(half, dtype=jnp.float32) / half)
    cos, sin = jnp.cos(angle)[:, None], jnp.sin(angle)[:, None]
    a, b = t[..., :half].astype(jnp.float32), t[..., half:].astype(jnp.float32)
    return jnp.concatenate([a * cos - b * sin, b * cos + a * sin], -1).astype(jnp.bfloat16)


def matmul(a, w):
    return jnp.dot(a, w, preferred_element_type=jnp.float32).astype(jnp.bfloat16)


def einsum(form, a, b):
    return jnp.einsum(form, a.astype(jnp.float32), b.astype(jnp.float32))


def attention(q, k, v):
    scores = einsum("tgsd,ugd->gstu", q, k) * q.shape[-1] ** -0.5
    token = jnp.arange(q.shape[0])
    scores = jnp.where(token[:, None] >= token, scores, -jnp.inf)
    weights = jax.nn.softmax(scores, -1).astype(jnp.bfloat16)
    return einsum("gstu,ugd->tgsd", weights, v).astype(jnp.bfloat16)


def one(x, gain_a, wq, wk, wv, wo, gain_m, w_gate, w_up, w_down):
    rows = x.shape[0]
    a, place = normed(x, gain_a), jnp.arange(rows)
    k = turned(matmul(a, wk).reshape(rows, -1, HEAD), place, THETA)
    q = turned(matmul(a, wq).reshape(rows, -1, HEAD), place, THETA).reshape(rows, k.shape[1], -1, HEAD)
    v = matmul(a, wv).reshape(rows, -1, HEAD)
    seen = attention(q, k, v).reshape(rows, -1)
    h = (x.astype(jnp.float32) + jnp.dot(seen, wo, preferred_element_type=jnp.float32)).astype(jnp.bfloat16)
    b = normed(h, gain_m)
    gate = jnp.dot(b, w_gate, preferred_element_type=jnp.float32)
    up = jnp.dot(b, w_up, preferred_element_type=jnp.float32)
    hidden = (jax.nn.silu(gate) * up).astype(jnp.bfloat16)
    return (h.astype(jnp.float32) + jnp.dot(hidden, w_down, preferred_element_type=jnp.float32)).astype(jnp.bfloat16)


def reference(x, gain_a, wq, wk, wv, wo, gain_m, w_gate, w_up, w_down):
    return lax.map(lambda sequence: one(sequence, gain_a, wq, wk, wv, wo, gain_m, w_gate, w_up, w_down), x)
```

```python
import functools

import jax
import jax.numpy as jnp
from jax import lax
from jax.experimental import pallas as pl
from jax.experimental.pallas import tpu as pltpu
from jax.sharding import PartitionSpec as P


HEAD = 128
THETA = 10000
LOG2E = 1.4426950408889634
VMEM = 60 * 2**20


def _dot(a, b, ca=1, cb=0):
    return lax.dot_general(a, b, (((ca,), (cb,)), ((), ())), preferred_element_type=jnp.float32)


def _norm(t, gain):
    return (t * lax.rsqrt(jnp.mean(t * t, -1, keepdims=True) + 1e-6) * gain).astype(jnp.bfloat16)


def _params(*semantics, limit=VMEM):
    return pltpu.CompilerParams(dimension_semantics=semantics or ("arbitrary",), vmem_limit_bytes=limit)


def _cost(flops, bytes_accessed):
    return pl.CostEstimate(flops=int(flops), transcendentals=0, bytes_accessed=int(bytes_accessed))


def _attention(q_s, kv_s, cos, sin, seen_s, block):
    tokens = kv_s.shape[0]

    def turned(t):
        t = t.astype(jnp.float32)
        return (t * cos + pltpu.roll(t, HEAD // 2, 1) * sin).astype(jnp.bfloat16)

    k, vt = turned(kv_s[:, :HEAD]), kv_s[:, HEAD:].T
    e = HEAD**-0.5 * LOG2E
    for n in range(q_s.shape[1] // HEAD):
        at = slice(n * HEAD, (n + 1) * HEAD)
        q = turned(q_s[:, at])
        for first in range(0, tokens, block):
            end = first + block
            s = _dot(k[:end], q[first:end], 1, 1)
            key = lax.broadcasted_iota(jnp.int32, s.shape, 0)
            query = lax.broadcasted_iota(jnp.int32, s.shape, 1) + first
            s = jnp.where(query >= key, s, -1e30)
            p = jnp.exp2((s - s.max(axis=0, keepdims=True)) * e)
            total = p.sum(axis=0, keepdims=True)
            out = _dot(vt[:, :end], p.astype(jnp.bfloat16), 1, 0) * (1 / total)
            seen_s[first:end, at] = out.T.astype(seen_s.dtype)


def _first_kernel(x_ref, gain_ref, wq_ref, wk_ref, wv_ref, wo_ref, cos_ref, sin_ref, o_ref, a_s, q_s, kv_s, seen_s, *, steps, wide, strip, block):
    i = pl.program_id(0)

    @pl.when(i == 0)
    def _():
        gain = gain_ref[...].astype(jnp.float32)

        def rows(r, _):
            at = pl.ds(pl.multiple_of(r * strip, strip), strip)
            a_s[at, :] = _norm(x_ref[0, at, :].astype(jnp.float32), gain)
            return 0

        lax.fori_loop(0, a_s.shape[0] // strip, rows, 0)
        kv_s[...] = _dot(a_s[...], jnp.concatenate([wk_ref[...], wv_ref[...]], 1)).astype(kv_s.dtype)

    for n in range(steps):

        @pl.when(i == n)
        def _(n=n):
            q_s[:, n * wide : (n + 1) * wide] = _dot(a_s[...], wq_ref[...]).astype(q_s.dtype)

    @pl.when(i == steps - 1)
    def _():
        _attention(q_s, kv_s, cos_ref[...], sin_ref[...], seen_s, block)

    @pl.when(i >= steps)
    def _():
        o_ref[...] = _dot(seen_s[...], wo_ref[...]).astype(o_ref.dtype)


def first_half(x, n, gain, wq, wk, wv, wo, cos, sin, wide=256, out_wide=1024, strip=16, block=256):
    _, tokens, d = x.shape
    width = wq.shape[1]
    steps, outs = width // wide, d // out_wide
    whole = lambda a: pl.BlockSpec(a.shape, lambda i: (0,) * a.ndim, pipeline_mode=pl.Buffered(1))
    return pl.pallas_call(
        functools.partial(_first_kernel, steps=steps, wide=wide, strip=strip, block=block),
        grid=(steps + outs,),
        in_specs=[
            pl.BlockSpec((1, tokens, d), lambda i: (n, 0, 0), pipeline_mode=pl.Buffered(1)),
            whole(gain),
            pl.BlockSpec((d, wide), lambda i: (0, jnp.minimum(i, steps - 1))),
            whole(wk),
            whole(wv),
            pl.BlockSpec((width, out_wide), lambda i: (0, jnp.maximum(i - steps, 0))),
            whole(cos),
            whole(sin),
        ],
        out_specs=pl.BlockSpec((tokens, out_wide), lambda i: (0, jnp.maximum(i - steps, 0))),
        out_shape=jax.ShapeDtypeStruct((tokens, d), jnp.bfloat16),
        scratch_shapes=[
            pltpu.VMEM((tokens, d), jnp.bfloat16),
            pltpu.VMEM((tokens, width), jnp.bfloat16),
            pltpu.VMEM((tokens, 2 * HEAD), jnp.bfloat16),
            pltpu.VMEM((tokens, width), jnp.bfloat16),
        ],
        compiler_params=_params(),
        cost_estimate=_cost(2 * tokens * d * (2 * width + 2 * HEAD) * 1.3, 4 * tokens * d + 2 * d * (2 * width + 2 * HEAD)),
        name="first",
    )(x, gain, wq, wk, wv, wo, cos, sin)


def _gate_up_kernel(b_ref, wg_ref, wu_ref, *rest):
    o_ref = rest[-1] if len(rest) == 1 else rest[-2]
    gate = _dot(b_ref[...], wg_ref[...])
    up = _dot(b_ref[...], wu_ref[...])
    o_ref[...] = (jax.nn.silu(gate) * up).astype(o_ref.dtype)
    if len(rest) > 1:
        rest[-1][0] = rest[0][...]


def gate_up(b, w_gate, w_up, first=0, last=None, wide=256, part=None, y=None, shape=None, n=None):
    rows, d = b.shape
    count = (w_gate.shape[1] if last is None else last) - first
    steps, skip = count // wide, first // wide
    cols = pl.BlockSpec((d, wide), lambda i: (0, i + skip if skip else i))
    given, alias = [b, w_gate, w_up], {}
    in_specs = [pl.BlockSpec((rows, d), lambda i: (0, 0), pipeline_mode=pl.Buffered(1)), cols, cols]
    out_specs, out_shape = [pl.BlockSpec((rows, wide), lambda i: (0, i))], [jax.ShapeDtypeStruct((rows, count), jnp.bfloat16)]
    if part is not None:
        parts = max(m for m in (1, 2, 4, 8, 16) if m <= steps)
        strip = rows // parts
        given, in_specs = given + [part], in_specs + [pl.BlockSpec((strip, d), lambda i: (jnp.minimum(i, parts - 1), 0))]
        if y is not None:
            given, in_specs, alias = given + [y], in_specs + [pl.BlockSpec(memory_space=pl.ANY)], {4: 1}
        out_specs = out_specs + [pl.BlockSpec((1, strip, d), lambda i: (n, jnp.minimum(i, parts - 1), 0))]
        out_shape = out_shape + [jax.ShapeDtypeStruct(shape, jnp.bfloat16)]
    got = pl.pallas_call(
        _gate_up_kernel,
        grid=(steps,),
        in_specs=in_specs,
        out_specs=out_specs,
        out_shape=out_shape,
        input_output_aliases=alias,
        compiler_params=_params(),
        cost_estimate=_cost(4 * rows * d * count, 4 * d * count + 2 * rows * (d + count)),
        name="gate_up",
    )(*given)
    return got[0] if part is None else got


def _down_kernel(a_ref, w_ref, o_ref):
    o_ref[...] = _dot(a_ref[...], w_ref[...]).astype(o_ref.dtype)


def down(hidden, w, first=0, last=None, wide=512):
    rows, ff = hidden.shape
    count = (w.shape[1] if last is None else last) - first
    skip = first // wide
    return pl.pallas_call(
        _down_kernel,
        grid=(count // wide,),
        in_specs=[pl.BlockSpec((rows, ff), lambda i: (0, 0), pipeline_mode=pl.Buffered(1)), pl.BlockSpec((ff, wide), lambda i: (0, i + skip if skip else i))],
        out_specs=pl.BlockSpec((rows, wide), lambda i: (0, i)),
        out_shape=jax.ShapeDtypeStruct((rows, count), jnp.bfloat16),
        compiler_params=_params(),
        cost_estimate=_cost(2 * rows * count * ff, 2 * ff * count + 2 * rows * (ff + count)),
        name="down",
    )(hidden, w)


def _middle_kernel(me_ref, x_ref, s_ref, gain_ref, h_ref, b_ref):
    del me_ref
    h = (x_ref[0].astype(jnp.float32) + s_ref[...].astype(jnp.float32)).astype(jnp.bfloat16)
    h_ref[...] = h
    b_ref[...] = _norm(h.astype(jnp.float32), gain_ref[...].astype(jnp.float32))


def middle(x, n, me, total, gain, strip=16):
    rows, d = total.shape
    per = rows // strip
    piece = pl.BlockSpec((strip, d), lambda i, me: (i, 0))
    return pl.pallas_call(
        _middle_kernel,
        grid_spec=pltpu.PrefetchScalarGridSpec(
            num_scalar_prefetch=1,
            grid=(per,),
            in_specs=[pl.BlockSpec((1, strip, d), lambda i, me: (n, me[0] * per + i, 0)), piece, pl.BlockSpec((1, d), lambda i, me: (0, 0))],
            out_specs=[piece, piece],
        ),
        out_shape=[jax.ShapeDtypeStruct((rows, d), jnp.bfloat16)] * 2,
        compiler_params=_params(limit=VMEM),
        cost_estimate=_cost(10 * rows * d, 10 * rows * d),
        name="middle",
    )(me, x, total, gain)


def _finish_kernel(h_ref, s_ref, o_ref):
    o_ref[...] = (h_ref[...].astype(jnp.float32) + s_ref[...].astype(jnp.float32)).astype(jnp.bfloat16)


def finish(h, total, first=0, strip=16):
    rows, width = total.shape
    piece = pl.BlockSpec((strip, width), lambda i: (i, 0))
    return pl.pallas_call(
        _finish_kernel,
        grid=(rows // strip,),
        in_specs=[pl.BlockSpec((strip, width), lambda i: (i, first // width)), piece],
        out_specs=piece,
        out_shape=jax.ShapeDtypeStruct((rows, width), jnp.bfloat16),
        compiler_params=_params(limit=VMEM),
        cost_estimate=_cost(10 * rows * width, 6 * rows * width),
        name="finish",
    )(h, total)


def _place_kernel(*refs):
    refs[-1][0] = refs[0][...]


def place(y, shape, part, n, first=0, strip=128):
    rows, width = part.shape
    given, specs = [part], [pl.BlockSpec((strip, width), lambda i: (i, 0))]
    if y is not None:
        given, specs = [part, y], specs + [pl.BlockSpec(memory_space=pl.ANY)]
    return pl.pallas_call(
        _place_kernel,
        grid=(rows // strip,),
        in_specs=specs,
        out_specs=pl.BlockSpec((1, strip, width), lambda i: (n, i, first // width)),
        out_shape=jax.ShapeDtypeStruct(shape, jnp.bfloat16),
        input_output_aliases={} if y is None else {1: 0},
        compiler_params=_params(limit=VMEM),
        cost_estimate=_cost(2 * rows * width, 4 * rows * width),
        name="place",
    )(*given)


def rotary(tokens):
    half = HEAD // 2
    angle = jnp.arange(tokens, dtype=jnp.float32)[:, None] * THETA ** (-jnp.arange(half, dtype=jnp.float32) / half)
    cos, sin = jnp.cos(angle), jnp.sin(angle)
    return jnp.concatenate([cos, cos], -1), jnp.concatenate([-sin, sin], -1)


def _down_sum_kernel(ha_ref, hb_ref, w_ref, h_ref, o_ref, keep_s, out_s, in_s, hop_out_s, hop_in_s, y_s,
                     out_sem, in_sem, hop_sem, hop_got, ag_sem, ag_got, side_sem, side_got, *, tiles, chips, cores, live):
    j = pl.program_id(0)
    me = lax.axis_index("tp")
    chip, core = me // cores, me % cores
    other = chip * cores + (1 - core)
    wide = w_ref.shape[1]

    def device(c):
        return lax.rem(c + 2 * chips, chips) * cores + core

    def copy(src, dst, send, got, to):
        return pltpu.make_async_remote_copy(src_ref=src, dst_ref=dst, send_sem=send, recv_sem=got, device_id={"tp": to},
                                            device_id_type=pl.DeviceIdType.MESH)

    @pl.when(j == 0)
    def _():
        barrier = pltpu.get_barrier_semaphore()
        for to in (device(chip + 1), device(chip - 1), other):
            pl.semaphore_signal(barrier, inc=1, device_id={"tp": to}, device_id_type=pl.DeviceIdType.MESH)
        pl.semaphore_wait(barrier, 3)

    def across(u):
        return copy(out_s.at[u], in_s.at[u], out_sem.at[u], in_sem.at[u], other)

    def hop(u, s, way):
        return copy(hop_out_s.at[u, s], hop_in_s.at[u, s], hop_sem.at[u, s], hop_got.at[u, s], device(chip + way))

    def block(u, s, way):
        return y_s.at[u, device(chip - s * way)]

    def around(u, s, way):
        return copy(block(u, s, way), block(u, s, way), ag_sem.at[u, s], ag_got.at[u, s], device(chip + way))

    def aside(u, s, way):
        return copy(block(u, s, way), block(u, s, way), side_sem.at[u, s], side_got.at[u, s], other)

    def stage(delay):
        u = j - delay
        return u, 1 - 2 * lax.rem(u + 2 * live, 2)

    def at(delay):
        return pl.when((j >= delay) & (j < tiles + delay))

    def summed(u, c):
        c = lax.rem(c + 2 * chips, chips)
        return keep_s[lax.rem(u, live), c] + in_s[u, c].astype(jnp.float32)

    @at(2 * chips + 1)
    def _():
        u, way = stage(2 * chips + 1)
        for s in range(chips):
            aside(u, s, way).wait_recv()
        o_ref[...] = y_s[u].reshape(o_ref.shape)
        across(u).wait_send()
        for s in range(chips - 1):
            hop(u, s, way).wait_send()
            around(u, s, way).wait_send()
        for s in range(chips):
            aside(u, s, way).wait_send()

    for s in range(chips - 1, 0, -1):

        @at(chips + 1 + s)
        def _(s=s):
            u, way = stage(chips + 1 + s)
            around(u, s - 1, way).wait_recv()
            if s < chips - 1:
                around(u, s, way).start()
            aside(u, s, way).start()

    @at(chips + 1)
    def _():
        u, way = stage(chips + 1)
        hop(u, chips - 2, way).wait_recv()
        total = summed(u, chip) + hop_in_s[u, chips - 2].astype(jnp.float32)
        columns = pl.ds(pl.multiple_of(u * wide, wide), wide)
        y_s[u, me] = (h_ref[:, columns].astype(jnp.float32) + total).astype(y_s.dtype)
        around(u, 0, way).start()
        aside(u, 0, way).start()

    for s in range(chips - 2, -1, -1):

        @at(2 + s)
        def _(s=s):
            u, way = stage(2 + s)
            if s == 0:
                across(u).wait_recv()
            else:
                hop(u, s - 1, way).wait_recv()
            total = summed(u, chip - (s + 1) * way)
            if s > 0:
                total = total + hop_in_s[u, s - 1].astype(jnp.float32)
            hop_out_s[u, s] = total.astype(hop_out_s.dtype)
            hop(u, s, way).start()

    @pl.when(j < tiles)
    def _():
        half = ha_ref.shape[1]
        term = _dot(ha_ref[...], w_ref[:half, :]) + _dot(hb_ref[...], w_ref[half:, :])
        term = term.reshape(chips, cores, -1, wide)
        for c in range(chips):
            mine = jnp.where(core == 0, term[c, 0], term[c, 1])
            theirs = jnp.where(core == 0, term[c, 1], term[c, 0])
            keep_s[lax.rem(j, live), c] = mine
            out_s[j, c] = theirs.astype(out_s.dtype)
        across(j).start()


def down_sum(hidden_a, hidden_b, w, h, size, wide=512, cores=2):
    rows, _ = hidden_a.shape
    ff, d = w.shape
    chips, tiles = size // cores, d // wide
    piece = rows // size
    last = 2 * chips + 1
    live = chips + 2
    whole = lambda a: pl.BlockSpec(a.shape, lambda i: (0, 0), pipeline_mode=pl.Buffered(1))
    dma = lambda n: pltpu.SemaphoreType.DMA((tiles, n))
    rounds = lambda n: pltpu.VMEM((tiles, n, piece, wide), jnp.bfloat16)
    return pl.pallas_call(
        functools.partial(_down_sum_kernel, tiles=tiles, chips=chips, cores=cores, live=live),
        grid_spec=pltpu.PrefetchScalarGridSpec(
            num_scalar_prefetch=0,
            grid=(tiles + last,),
            in_specs=[whole(hidden_a), whole(hidden_b), pl.BlockSpec((ff, wide), lambda i: (0, jnp.minimum(i, tiles - 1))), whole(h)],
            out_specs=pl.BlockSpec((rows, wide), lambda i: (0, jnp.maximum(i - last, 0))),
            scratch_shapes=[
                pltpu.VMEM((live, chips, piece, wide), jnp.float32),
                rounds(chips), rounds(chips), rounds(chips - 1), rounds(chips - 1), rounds(size),
                pltpu.SemaphoreType.DMA((tiles,)), pltpu.SemaphoreType.DMA((tiles,)),
                dma(chips - 1), dma(chips - 1), dma(chips - 1), dma(chips - 1), dma(chips), dma(chips),
            ],
        ),
        out_shape=jax.ShapeDtypeStruct((rows, d), jnp.bfloat16),
        compiler_params=pltpu.CompilerParams(dimension_semantics=("arbitrary",), vmem_limit_bytes=VMEM, collective_id=0, has_side_effects=True),
        cost_estimate=_cost(2 * rows * ff * d, 2 * ff * d),
        name="down_sum",
    )(hidden_a, hidden_b, w, h)


def solution(mesh):
    size = mesh.shape["tp"]

    def step(x, gain_a, wq, wk, wv, wo, gain_m, w_gate, w_up, w_down):
        batch, rows, d = x.shape
        half = w_gate.shape[1] // 2
        gain_a, gain_m = gain_a.reshape(1, d), gain_m.reshape(1, d)
        me = lax.axis_index("tp").astype(jnp.int32).reshape(1)
        cos, sin = rotary(rows)

        def scatter(term):
            return lax.psum_scatter(term, "tp", scatter_dimension=0, tiled=True)

        def gather(piece):
            return lax.all_gather(piece, "tp", axis=0, tiled=True)

        h, b, parts = [None] * batch, [None] * batch, [None] * batch
        for n in range(batch):
            term = first_half(x, n, gain_a, wq, wk, wv, wo, cos, sin)
            total = scatter(term)
            h[n], piece = middle(x, n, me, total, gain_m)
            b[n] = gather(piece)
        for n in range(batch - 1):
            hidden = gate_up(b[n], w_gate, w_up)
            term = down(hidden, w_down)
            total = scatter(term)
            piece = finish(h[n], total)
            parts[n] = gather(piece)
        n = batch - 1
        hidden_a, y = gate_up(b[n], w_gate, w_up, 0, half, part=parts[0], shape=x.shape, n=0)
        hidden_b, y = gate_up(b[n], w_gate, w_up, half, 2 * half, part=parts[1], y=y, shape=x.shape, n=1)
        parts[n] = down_sum(hidden_a, hidden_b, w_down, h[n], size)
        for m in range(2, batch):
            y = place(y, x.shape, parts[m], m)
        return y

    tokens, whole, columns, rows_of = P("dp", None, None), P(None), P(None, "tp"), P("tp", None)
    return jax.shard_map(
        step,
        mesh=mesh,
        in_specs=(tokens, whole, columns, columns, columns, rows_of, whole, columns, columns, rows_of),
        out_specs=tokens,
        check_vma=False,
    )
```
